256 devices in a mesh: pairs: 32 (over x, y, core), aux: 8 (over z).
Axes of the slice: x: 4, y: 4, z: 8, core: 2. Of those that a mesh axis runs over, the one named last changes fastest.
Arguments:
- panels: bfloat16 [64, 28672, 256], P(None, ('pairs', 'aux')), may hold values from -0.59765625 to 0.59765625
- domain: int32 [32, 6], replicated, may hold values from 0 to 63, as said below
- pair_slots: int32 [384, 2], P('pairs'), may hold values from 0 to 5
- ranks: int32 [384, 2], P('pairs'), may hold values from 40 to 128
- transforms: bfloat16 [384, 2, 256, 128], P('pairs'), may hold values from -0.375 to 0.375
- trial: bfloat16 [384, 2, 128, 128], P('pairs'), may hold values from -0.5 to 0.5
Outputs:
- sigma: bfloat16 [384, 2, 128, 128], P('pairs', None, 'aux')
The draws below stay inside these ranges and needn't reach their ends.
Inputs may be any that keep to these rules, and one draw needn't show every extreme that they name: `domain`: each row holds 6 different LMO numbers.
All inputs are finite; a program needn't handle non-finite values.
Results may differ from the reference program's by a relative error of at most 0.0039.
Values may be sent and summed in bfloat16 or wider, within the bound.
A program may use at most 128 MiB of HBM per device.

```python
import jax
import jax.numpy as jnp
from jax import lax

NV = 256
R = 128
ROOTS = 2
NOCC = 64
LSLOT = 6
PAIR_DEV = 12
NAUX = 28672
GROUPS = 32
PAIRS = 384


def draw_domain(key, part):
    keys = jax.random.split(jax.random.fold_in(key, 11), GROUPS)
    rows = jax.vmap(lambda single: jax.random.permutation(single, NOCC)[:LSLOT])(keys)
    return rows.astype(jnp.int32)


def place_ends(drawn, stream_key, smallest, largest):
    longest = drawn.shape.index(max(drawn.shape))
    spots = []
    for shift in (0, 1):
        where = [jax.random.randint(jax.random.fold_in(stream_key, axis), (), 0, length) for axis, length in enumerate(drawn.shape)]
        where[longest] = (where[longest] + shift) % drawn.shape[longest]
        spots.append(tuple(where))
    return drawn.at[spots[0]].set(smallest).at[spots[1]].set(largest)


def steps_of(rng, shape, cuts, least, largest):
    gain, own = 1.0, jax.random.fold_in(rng, 6)
    for axis_at, parts in cuts:
        draws = jnp.exp(jax.random.uniform(jax.random.fold_in(own, axis_at), (parts,), jnp.float32, least / len(cuts), largest / len(cuts)))
        gain = gain * jnp.repeat(draws, shape[axis_at] // parts).reshape([-1 if axis == axis_at else 1 for axis in range(len(shape))])
    return gain


def normal_values(rng, extent, deviation, reach, cuts=(), held_as=jnp.bfloat16):
    values = deviation * jax.random.normal(rng, extent, jnp.float32)
    if cuts:
        values = values * steps_of(rng, extent, cuts, -0.22, 0.18)
    return jnp.clip(values, -reach, reach).astype(held_as)


def setup_inputs(seed: int = 0) -> dict:
    key_of = jax.random.split(jax.random.key(seed), 7)
    panels = normal_values(key_of[0], (NOCC, NAUX, NV), 0.08, 0.59765625, ((1, 256),))
    domain = draw_domain(jax.random.fold_in(key_of[6], 71), 0)
    pair_slots = place_ends(jax.random.randint(key_of[2], (PAIRS, 2), 0, LSLOT), jax.random.fold_in(key_of[2], 1), 0, LSLOT - 1).astype(jnp.int32)
    ranks = place_ends(jax.random.randint(key_of[3], (PAIRS, ROOTS), R * 5 // 16, R + 1), jax.random.fold_in(key_of[3], 1), R * 5 // 16, R).astype(jnp.int32)
    transforms = normal_values(key_of[4], (PAIRS, ROOTS, NV, R), NV ** -0.5, 0.375, ((0, 32),))
    trial = normal_values(key_of[5], (PAIRS, ROOTS, R, R), R ** -0.5, 0.5, ((0, 32),))
    return {"panels": panels, "domain": domain, "pair_slots": pair_slots, "ranks": ranks, "transforms": transforms, "trial": trial}


def reference(panels, domain, pair_slots, ranks, transforms, trial):
    positions = jnp.arange(R, dtype=jnp.int32)

    def one_pair(index):
        group = index // PAIR_DEV
        lmo_ids = domain[group][pair_slots[index]]
        left = panels[lmo_ids[0]].astype(jnp.float32)
        right = panels[lmo_ids[1]].astype(jnp.float32)
        keep = (positions[None, :] < ranks[index][:, None]).astype(jnp.float32)
        coeffs = transforms[index].astype(jnp.float32) * keep[:, None, :]
        amplitude = trial[index].astype(jnp.float32) * keep[:, :, None] * keep[:, None, :]
        left_proj = jnp.einsum('qv,svr->sqr', left, coeffs, precision=lax.Precision.HIGHEST).astype(jnp.bfloat16)
        right_proj = jnp.einsum('qv,svr->sqr', right, coeffs, precision=lax.Precision.HIGHEST).astype(jnp.bfloat16)
        left_proj, right_proj = lax.optimization_barrier((left_proj, right_proj))
        kmat = jnp.einsum('sqa,sqb->sab', left_proj.astype(jnp.float32), right_proj.astype(jnp.float32), precision=lax.Precision.HIGHEST)
        with_right = jnp.einsum('sab,sbc->sac', kmat, amplitude, precision=lax.Precision.HIGHEST)
        with_left = jnp.einsum('sac,sbc->sab', amplitude, kmat, precision=lax.Precision.HIGHEST)
        return (kmat + with_right + with_left).astype(jnp.bfloat16)

    return lax.map(one_pair, jnp.arange(PAIRS, dtype=jnp.int32))
```

```python
import jax
import jax.numpy as jnp
from jax import lax
from jax.experimental import pallas as pl
from jax.experimental.pallas import tpu as pltpu
from jax.sharding import PartitionSpec as P

MESH = pl.DeviceIdType.MESH
NX, NY, NZ = 4, 4, 8
ROOTS = 2
ORDER = (2, 1, 3, 0)
F32, BF16 = jnp.float32, jnp.bfloat16
TRANS_A = (((0,), (0,)), ((), ()))
TRANS_B = (((1,), (1,)), ((), ()))


def split(value):
    high = value.astype(BF16)
    return high, (value - high.astype(F32)).astype(BF16)


def dot(a, b, dims=(((1,), (0,)), ((), ()))):
    return lax.dot_general(a, b, dims, preferred_element_type=F32)


def kernel(
    domain, ranks, panels, slots_in, transforms, trial, out,
    recv0, recv1, recv2, recv3, stage, slots_v, slots_s,
    gown, gsend1, gsend2, gsend3, grecv1, grecv2, grecv3,
    sig_f, sig_b, zrecv,
    send_sem, recv_sem, slot_send, slot_recv, slot_local, gs_sem, gr_sem, zs_sem, zr_sem,
):
    pairs = out.shape[0]
    rows = panels.shape[1]
    lslot = domain.shape[1]
    recvs = (recv0, recv1, recv2, recv3)
    gsends = (None, gsend1, gsend2, gsend3)
    grecvs = (None, grecv1, grecv2, grecv3)
    pos = lax.axis_index("pairs")
    z = lax.axis_index("aux")
    x, y, c = pos // (2 * NY), (pos // 2) % NY, pos % 2

    def place(x2, y2, c2):
        return (x2 % NX) * (2 * NY) + (y2 % NY) * 2 + c2

    def same(m):
        return x + m * (1 - c), y + m * c, c

    def other(m):
        return x + m * c, y + m * (1 - c), 1 - c

    def other_source(m):
        return x + m * (1 - c), y + m * c, 1 - c

    def peer(r):
        return x + r * c, y + r * (1 - c), c

    def group_of(dest, r):
        x2, y2, c2 = dest
        return place(x2 + r * c2, y2 + r * (1 - c2), c2)

    barrier = pltpu.get_barrier_semaphore()
    greeted = 0
    for target in (
        [(place(*same(m)), z) for m in range(1, 4)]
        + [(place(*other(m)), z) for m in range(4)]
        + [(place(*other_source(m)), z) for m in range(1, 4)]
        + [(place(*peer(r)), z) for r in range(1, 4)]
        + [(pos, (z + k) % NZ) for k in range(1, NZ)]
    ):
        pl.semaphore_signal(barrier, inc=1, device_id=target, device_id_type=MESH)
        greeted += 1

    dests = [(same(m), 2 * m) for m in range(1, 4)] + [(other(m), 2 * m + 1) for m in range(4)]
    dests = [dests[k] for k in (1, 5, 0, 2, 4, 6, 3)]

    def fill(dest, r, k):
        group = group_of(dest, r)

        def body(s, carry):
            stage[k, r, s] = panels[domain[group, s]]
            return carry

        lax.fori_loop(0, lslot, body, 0)

    def panel_copy(dest, block, r, k):
        return pltpu.make_async_remote_copy(
            src_ref=stage.at[k, r],
            dst_ref=recvs[r].at[:, pl.ds(block * rows, rows), :],
            send_sem=send_sem.at[r, k],
            recv_sem=recv_sem.at[r, k],
            device_id=(place(*dest), z),
            device_id_type=MESH,
        )

    def slot_copy(r):
        return pltpu.make_async_remote_copy(
            src_ref=slots_in,
            dst_ref=slots_v.at[r],
            send_sem=slot_send.at[r],
            recv_sem=slot_recv.at[r],
            device_id=(place(*peer(NX - r)), z),
            device_id_type=MESH,
        )

    work = [(r, k) for r in ORDER for k in range(len(dests))]
    fill(dests[0][0], ORDER[0], 0)
    fill(dests[1][0], ORDER[0], 1)
    pl.semaphore_wait(barrier, greeted)
    for r in range(1, 4):
        slot_copy(r).start()
    for n, (r, k) in enumerate(work):
        if n + 2 < len(work):
            r2, k2 = work[n + 2]
            fill(dests[k2][0], r2, k2)
        panel_copy(*dests[k], r, k).start()
    for r in ORDER:
        group = group_of((x, y, c), r)

        def own(s, carry, group=group, r=r):
            recvs[r][s, 0:rows, :] = panels[domain[group, s]]
            return carry

        lax.fori_loop(0, lslot, own, 0)
    for r in range(4):
        if r:
            slot_copy(r).wait()
        local = pltpu.make_async_copy(slots_v.at[r] if r else slots_in, slots_s.at[r], slot_local.at[r])
        local.start()
        local.wait()

    half = pairs // 2

    def g_copy(r, h):
        part = pl.ds(h * half, half)
        return pltpu.make_async_remote_copy(
            src_ref=gsends[r].at[part],
            dst_ref=grecvs[r].at[part],
            send_sem=gs_sem.at[r, h],
            recv_sem=gr_sem.at[r, h],
            device_id=(place(*peer(r)), z),
            device_id_type=MESH,
        )

    def gram(r, p):
        left = recvs[r][slots_s[r, 0, 2 * p]]
        right = recvs[r][slots_s[r, 0, 2 * p + 1]]
        return dot(left, right, TRANS_A)

    for r in ORDER:
        for k in range(len(dests)):
            panel_copy(*dests[k], r, k).wait_recv()
        if r:
            for h in range(2):
                def send_body(p, carry, r=r):
                    gsends[r][p] = gram(r, p).astype(BF16)
                    return carry

                lax.fori_loop(h * half, (h + 1) * half, send_body, 0)
                g_copy(r, h).start()
        else:
            def own_body(p, carry):
                gown[p] = gram(0, p)
                return carry

            lax.fori_loop(0, pairs, own_body, 0)

    def z_copy(k, h):
        part = pl.ds(h * half, half)
        to = (z + k) % NZ
        piece = out.shape[2]
        return pltpu.make_async_remote_copy(
            src_ref=sig_b.at[part, :, pl.ds(pl.multiple_of(to * piece, piece), piece), :],
            dst_ref=zrecv.at[k, part],
            send_sem=zs_sem.at[k, h],
            recv_sem=zr_sem.at[k, h],
            device_id=(pos, to),
            device_id_type=MESH,
        )

    rank = trial.shape[3]
    row_at = lax.broadcasted_iota(jnp.int32, (rank, rank), 0)
    col_at = lax.broadcasted_iota(jnp.int32, (rank, rank), 1)
    for h in range(2):
        for r in range(1, 4):
            g_copy(r, h).wait_recv()

        def sigma_body(p, carry):
            total = gown[p]
            for r in range(1, 4):
                total = total + grecvs[r][p].astype(F32)
            coeffs = jnp.concatenate([transforms[p, 0], transforms[p, 1]], axis=1)
            g_high, g_low = split(total)
            t = dot(g_high, coeffs) + dot(g_low, coeffs)
            t_high, t_low = split(t)
            for root in range(ROOTS):
                cols = slice(root * rank, (root + 1) * rank)
                d = transforms[p, root]
                keep = (row_at < ranks[p, root]) & (col_at < ranks[p, root])
                kmat = dot(d, t_high[:, cols], TRANS_A) + dot(d, t_low[:, cols], TRANS_A)
                kmat = jnp.where(keep, kmat, 0.0)
                amp = jnp.where(keep, trial[p, root].astype(F32), 0.0).astype(BF16)
                k_high, k_low = split(kmat)
                sig = kmat + (dot(k_high, amp) + dot(k_low, amp))
                sig = sig + (dot(amp, k_high, TRANS_B) + dot(amp, k_low, TRANS_B))
                sig_f[p, root] = sig
                sig_b[p, root] = sig.astype(BF16)
            return carry

        lax.fori_loop(h * half, (h + 1) * half, sigma_body, 0)
        for k in (4, 3, 5, 2, 6, 1, 7):
            z_copy(k, h).start()

    piece = out.shape[2]
    for h in range(2):
        for k in range(1, NZ):
            z_copy(k, h).wait_recv()

        def sum_body(p, carry):
            for root in range(ROOTS):
                total = sig_f[p, root, pl.ds(pl.multiple_of(z * piece, piece), piece), :]
                for k in range(1, NZ):
                    total = total + zrecv[k, p, root].astype(F32)
                out[p, root] = total.astype(BF16)
            return carry

        lax.fori_loop(h * half, (h + 1) * half, sum_body, 0)

    for r in ORDER:
        for k in range(len(dests)):
            panel_copy(*dests[k], r, k).wait_send()
    for h in range(2):
        for r in range(1, 4):
            g_copy(r, h).wait_send()
        for k in range(1, NZ):
            z_copy(k, h).wait_send()


def per_device(panels, domain, pair_slots, ranks, transforms, trial):
    pairs, roots, width, rank = transforms.shape
    rows, lslot = panels.shape[1], domain.shape[1]
    flat = pair_slots.reshape(1, -1)
    slots_in = jnp.pad(flat, ((0, 7), (0, 128 - flat.shape[1])))
    smem = pl.BlockSpec(memory_space=pltpu.SMEM)
    vmem = pl.BlockSpec(memory_space=pltpu.VMEM)
    dma = pltpu.SemaphoreType.DMA
    return pl.pallas_call(
        kernel,
        name="sigma",
        out_shape=jax.ShapeDtypeStruct((pairs, roots, rank // NZ, rank), BF16),
        in_specs=[smem, smem, vmem, vmem, vmem, vmem],
        out_specs=vmem,
        scratch_shapes=[pltpu.VMEM((lslot, 8 * rows, width), BF16)] * 4
        + [
            pltpu.VMEM((7, 4, lslot, rows, width), BF16),
            pltpu.VMEM((4, 8, 128), jnp.int32),
            pltpu.SMEM((4, 8, 128), jnp.int32),
            pltpu.VMEM((pairs, width, width), F32),
        ]
        + [pltpu.VMEM((pairs, width, width), BF16)] * 6
        + [
            pltpu.VMEM((pairs, roots, rank, rank), F32),
            pltpu.VMEM((pairs, roots, rank, rank), BF16),
            pltpu.VMEM((NZ, pairs, roots, rank // NZ, rank), BF16),
            dma((4, 7)),
            dma((4, 7)),
            dma((4,)),
            dma((4,)),
            dma((4,)),
            dma((4, 2)),
            dma((4, 2)),
            dma((NZ, 2)),
            dma((NZ, 2)),
        ],
        compiler_params=pltpu.CompilerParams(
            collective_id=0, has_side_effects=True, vmem_limit_bytes=63 * 2**20
        ),
    )(domain, ranks, panels, slots_in, transforms, trial)


def solution(mesh):
    return jax.shard_map(
        per_device,
        mesh=mesh,
        in_specs=(
            P(None, ("pairs", "aux"), None),
            P(),
            P("pairs", None),
            P("pairs", None),
            P("pairs", None, None, None),
            P("pairs", None, None, None),
        ),
        out_specs=P("pairs", None, "aux", None),
        check_vma=False,
    )
```

```python
import jax
import jax.numpy as jnp
from jax import lax
from jax.experimental import pallas as pl
from jax.experimental.pallas import tpu as pltpu
from jax.sharding import PartitionSpec as P

MESH = pl.DeviceIdType.MESH
NX, NY, NZ = 4, 4, 8
ROOTS = 2
ORDER = (2, 1, 3, 0)
CHUNKS = 4
F32, BF16 = jnp.float32, jnp.bfloat16
PLAIN = (((1,), (0,)), ((), ()))
TRANS_A = (((0,), (0,)), ((), ()))
TRANS_B = (((1,), (1,)), ((), ()))


def split(value):
    high = value.astype(BF16)
    return high, (value - high.astype(F32)).astype(BF16)


def dot(a, b, dims=PLAIN):
    return lax.dot_general(a, b, dims, preferred_element_type=F32)


def kernel(
    domain, ranks, slots_in, panels_in, transforms_in, trial_in, out,
    panels, transforms, trial,
    recv0, recv1, recv2, recv3, stage, slots_v, slots_s, dall, gram,
    kown, ksend, krecv, sig_f, sig_b, zrecv,
    in_sem, send_sem, recv_sem, slot_send, slot_recv, slot_local,
    ds_sem, dr_sem, rs_sem, rr_sem, ls_sem, lr_sem,
    ks_sem, kr_sem, zs_sem, zr_sem,
):
    pairs, piece, rank = out.shape[0], out.shape[2], out.shape[3]
    rows = panels.shape[1]
    lslot = domain.shape[0]
    width = transforms.shape[1]
    recvs = (recv0, recv1, recv2, recv3)
    pos = lax.axis_index("pairs")
    z = lax.axis_index("aux")
    x, y, c = pos // (2 * NY), (pos // 2) % NY, pos % 2

    loads = [
        pltpu.make_async_copy(src, dst, in_sem.at[n])
        for n, (src, dst) in enumerate(
            ((panels_in, panels), (transforms_in, transforms), (trial_in, trial))
        )
    ]
    for load in loads:
        load.start()

    def place(x2, y2, c2):
        return (x2 % NX) * (2 * NY) + (y2 % NY) * 2 + c2

    def same(m):
        return x + m * (1 - c), y + m * c, c

    def other(m):
        return x + m * c, y + m * (1 - c), 1 - c

    def other_source(m):
        return x + m * (1 - c), y + m * c, 1 - c

    def peer(r):
        return x + r * c, y + r * (1 - c), c

    def group_of(dest, r):
        x2, y2, c2 = dest
        return place(x2 + r * c2, y2 + r * (1 - c2), c2)

    barrier = pltpu.get_barrier_semaphore()
    greeted = 0
    for target in (
        [(place(*same(m)), z) for m in range(1, 4)]
        + [(place(*other(m)), z) for m in range(4)]
        + [(place(*other_source(m)), z) for m in range(1, 4)]
        + [(place(*peer(r)), z) for r in range(1, 4)]
        + [(pos, (z + k) % NZ) for k in range(1, NZ)]
    ):
        pl.semaphore_signal(barrier, inc=1, device_id=target, device_id_type=MESH)
        greeted += 1

    dests = [(same(m), 2 * m) for m in range(1, 4)] + [(other(m), 2 * m + 1) for m in range(4)]
    dests = [dests[k] for k in (1, 5, 0, 2, 4, 6, 3)]

    def fill(dest, r, k):
        group = group_of(dest, r)
        for s in range(lslot):
            stage[k, r, s] = panels[domain[s, group]]

    def panel_copy(dest, block, r, k):
        return pltpu.make_async_remote_copy(
            src_ref=stage.at[k, r],
            dst_ref=recvs[r].at[:, pl.ds(block * rows, rows), :],
            send_sem=send_sem.at[r, k],
            recv_sem=recv_sem.at[r, k],
            device_id=(place(*dest), z),
            device_id_type=MESH,
        )

    def slot_copy(r):
        return pltpu.make_async_remote_copy(
            src_ref=slots_in,
            dst_ref=slots_v.at[r],
            send_sem=slot_send.at[r],
            recv_sem=slot_recv.at[r],
            device_id=(place(*peer(NX - r)), z),
            device_id_type=MESH,
        )

    part = width // NZ

    def part_of(origin):
        return pl.ds(pl.multiple_of((origin % NZ) * part, part), part)

    def d_copy(r):
        return pltpu.make_async_remote_copy(
            src_ref=transforms.at[:, part_of(z), :],
            dst_ref=dall.at[r - 1, :, part_of(z), :],
            send_sem=ds_sem.at[r],
            recv_sem=dr_sem.at[r],
            device_id=(place(*peer(NX - r)), z),
            device_id_type=MESH,
        )

    def ring_copy(way, step):
        origin = part_of(z - way * step + NZ)
        chosen = slice(None)
        if step == NZ // 2 - 1:
            chosen = pl.ds(0, 2) if way == 1 else pl.ds(2, 1)
        send, recv = (rs_sem, rr_sem) if way == 1 else (ls_sem, lr_sem)
        ref = dall.at[chosen, :, origin, :]
        return pltpu.make_async_remote_copy(
            src_ref=ref,
            dst_ref=ref,
            send_sem=send.at[step],
            recv_sem=recv.at[step],
            device_id=(pos, (z + way + NZ) % NZ),
            device_id_type=MESH,
        )

    def ring(step):
        for way in (1, -1):
            if step:
                ring_copy(way, step - 1).wait_recv()
            if step < NZ // 2:
                ring_copy(way, step).start()

    work = [(r, k) for r in ORDER for k in range(len(dests))]
    loads[0].wait()
    fill(dests[0][0], ORDER[0], 0)
    fill(dests[1][0], ORDER[0], 1)
    loads[1].wait()
    pl.semaphore_wait(barrier, greeted)
    for r in (2, 1, 3):
        d_copy(r).start()
    for r in range(1, 4):
        slot_copy(r).start()
    for n, (r, k) in enumerate(work):
        if n + 2 < len(work):
            r2, k2 = work[n + 2]
            fill(dests[k2][0], r2, k2)
        panel_copy(*dests[k], r, k).start()
    for r in ORDER:
        group = group_of((x, y, c), r)
        for s in range(lslot):
            recvs[r][s, 0:rows, :] = panels[domain[s, group]]
    for r in range(1, 4):
        d_copy(r).wait_recv()
    ring(0)
    for r in range(4):
        if r:
            slot_copy(r).wait()
        local = pltpu.make_async_copy(slots_v.at[r] if r else slots_in, slots_s.at[r], slot_local.at[r])
        local.start()
        local.wait()
    loads[2].wait()

    def wait_panels(r):
        for k in range(len(dests)):
            panel_copy(*dests[k], r, k).wait_recv()

    def grams(r):
        def body(p, carry):
            left = recvs[r][slots_s[r, 0, p]]
            right = recvs[r][slots_s[r, 1, p]]
            gram[r, p] = dot(left, right, TRANS_A)
            return carry

        lax.fori_loop(0, pairs, body, 0)

    def k_of(r, p, d0, d1):
        g_high, g_low = split(gram[r, p])
        coeffs = jnp.concatenate([d0, d1], axis=1)
        t_high, t_low = split(dot(g_high, coeffs) + dot(g_low, coeffs))
        result = []
        for root, d in enumerate((d0, d1)):
            cols = slice(root * rank, (root + 1) * rank)
            both = jnp.concatenate([t_high[:, cols], t_low[:, cols]], axis=1)
            summed = dot(d, both, TRANS_A)
            result.append(summed[:, :rank] + summed[:, rank:])
        return result

    per = pairs // CHUNKS

    def k_copy(r, h):
        some = pl.ds(h * per, per)
        return pltpu.make_async_remote_copy(
            src_ref=ksend.at[r - 1, some],
            dst_ref=krecv.at[r - 1, some],
            send_sem=ks_sem.at[r - 1, h],
            recv_sem=kr_sem.at[r - 1, h],
            device_id=(place(*peer(r)), z),
            device_id_type=MESH,
        )

    wait_panels(2)
    ring(1)
    grams(2)
    ring(2)
    wait_panels(1)
    grams(1)
    ring(3)
    wait_panels(3)
    grams(3)
    ring(4)

    def k_chunk(h, carry):
        for r in (2, 1, 3):
            for n in range(per):
                p = h * per + n
                mats = k_of(r, p, dall[r - 1, ROOTS * p], dall[r - 1, ROOTS * p + 1])
                for root in range(ROOTS):
                    ksend[r - 1, p, root] = mats[root].astype(BF16)
        for r in (2, 1, 3):
            k_copy(r, h).start()
        return carry

    lax.fori_loop(0, CHUNKS, k_chunk, 0)
    wait_panels(0)
    grams(0)

    def own_chunk(h, carry):
        for n in range(per):
            p = h * per + n
            mats = k_of(0, p, transforms[ROOTS * p], transforms[ROOTS * p + 1])
            for root in range(ROOTS):
                kown[p, root] = mats[root]
        return carry

    lax.fori_loop(0, CHUNKS, own_chunk, 0)

    def z_copy(k, h):
        some = pl.ds(h * per, per)
        to = (z + k) % NZ
        return pltpu.make_async_remote_copy(
            src_ref=sig_b.at[some, :, pl.ds(pl.multiple_of(to * piece, piece), piece), :],
            dst_ref=zrecv.at[k, some],
            send_sem=zs_sem.at[k, h],
            recv_sem=zr_sem.at[k, h],
            device_id=(pos, to),
            device_id_type=MESH,
        )

    row_at = lax.broadcasted_iota(jnp.int32, (rank, rank), 0)
    col_at = lax.broadcasted_iota(jnp.int32, (rank, rank), 1)

    def sigma_chunk(h, carry):
        for r in range(1, 4):
            k_copy(r, h).wait_recv()
        for n in range(per):
            p = h * per + n
            for root in range(ROOTS):
                kmat = kown[p, root]
                for r in range(1, 4):
                    kmat = kmat + krecv[r - 1, p, root].astype(F32)
                keep = (row_at < ranks[root, p]) & (col_at < ranks[root, p])
                kmat = jnp.where(keep, kmat, 0.0)
                amp = jnp.where(keep, trial[p, root].astype(F32), 0.0).astype(BF16)
                both = jnp.concatenate(split(kmat), axis=1)
                sig = kmat + dot(both, jnp.concatenate([amp, amp], axis=0))
                sig = sig + dot(jnp.concatenate([amp, amp], axis=1), both, TRANS_B)
                sig_f[p, root] = sig
                sig_b[p, root] = sig.astype(BF16)
        for k in (4, 3, 5, 2, 6, 1, 7):
            z_copy(k, h).start()
        return carry

    lax.fori_loop(0, CHUNKS, sigma_chunk, 0)

    def sum_chunk(h, carry):
        for k in range(1, NZ):
            z_copy(k, h).wait_recv()
        for n in range(per):
            p = h * per + n
            for root in range(ROOTS):
                total = sig_f[p, root, pl.ds(pl.multiple_of(z * piece, piece), piece), :]
                for k in range(1, NZ):
                    total = total + zrecv[k, p, root].astype(F32)
                out[p, root] = total.astype(BF16)
        return carry

    lax.fori_loop(0, CHUNKS, sum_chunk, 0)

    for r in ORDER:
        for k in range(len(dests)):
            panel_copy(*dests[k], r, k).wait_send()
    for r in range(1, 4):
        d_copy(r).wait_send()
    for step in range(NZ // 2):
        for way in (1, -1):
            ring_copy(way, step).wait_send()
    for h in range(CHUNKS):
        for r in range(1, 4):
            k_copy(r, h).wait_send()
        for k in range(1, NZ):
            z_copy(k, h).wait_send()


def per_device(panels, domain, pair_slots, ranks, transforms, trial):
    pairs, roots, width, rank = transforms.shape
    occ, rows, _ = panels.shape
    lslot = domain.shape[1]
    smem = pl.BlockSpec(memory_space=pltpu.SMEM)
    vmem = pl.BlockSpec(memory_space=pltpu.VMEM)
    far = pl.BlockSpec(memory_space=pl.ANY)
    dma = pltpu.SemaphoreType.DMA
    return pl.pallas_call(
        kernel,
        name="sigma",
        out_shape=jax.ShapeDtypeStruct((pairs, roots, rank // NZ, rank), BF16),
        in_specs=[smem, smem, vmem, far, far, far],
        out_specs=vmem,
        scratch_shapes=[
            pltpu.VMEM((occ, rows, width), BF16),
            pltpu.VMEM((pairs * roots, width, rank), BF16),
            pltpu.VMEM((pairs, roots, rank, rank), BF16),
        ]
        + [pltpu.VMEM((lslot, 8 * rows, width), BF16)] * 4
        + [
            pltpu.VMEM((7, 4, lslot, rows, width), BF16),
            pltpu.VMEM((4, 2, pairs), jnp.int32),
            pltpu.SMEM((4, 2, pairs), jnp.int32),
            pltpu.VMEM((3, pairs * roots, width, rank), BF16),
            pltpu.VMEM((4, pairs, width, width), F32),
            pltpu.VMEM((pairs, roots, rank, rank), F32),
            pltpu.VMEM((3, pairs, roots, rank, rank), BF16),
            pltpu.VMEM((3, pairs, roots, rank, rank), BF16),
            pltpu.VMEM((pairs, roots, rank, rank), F32),
            pltpu.VMEM((pairs, roots, rank, rank), BF16),
            pltpu.VMEM((NZ, pairs, roots, rank // NZ, rank), BF16),
            dma((3,)),
            dma((4, 7)),
            dma((4, 7)),
            dma((4,)),
            dma((4,)),
            dma((4,)),
            dma((4,)),
            dma((4,)),
            dma((4,)),
            dma((4,)),
            dma((4,)),
            dma((4,)),
            dma((3, CHUNKS)),
            dma((3, CHUNKS)),
            dma((NZ, CHUNKS)),
            dma((NZ, CHUNKS)),
        ],
        compiler_params=pltpu.CompilerParams(
            collective_id=0, has_side_effects=True, vmem_limit_bytes=67043328
        ),
    )(
        domain.T,
        ranks.T,
        pair_slots.T,
        panels,
        transforms.reshape(pairs * roots, width, rank),
        trial,
    )


def solution(mesh):
    return jax.shard_map(
        per_device,
        mesh=mesh,
        in_specs=(
            P(None, ("pairs", "aux"), None),
            P(),
            P("pairs", None),
            P("pairs", None),
            P("pairs", None, None, None),
            P("pairs", None, None, None),
        ),
        out_specs=P("pairs", None, "aux", None),
        check_vma=False,
    )
```

```python
import jax
import jax.numpy as jnp
from jax import lax
from jax.experimental import pallas as pl
from jax.experimental.pallas import tpu as pltpu
from jax.sharding import PartitionSpec as P

MESH = pl.DeviceIdType.MESH
NX, NY, NZ = 4, 4, 8
ROOTS = 2
ORDER = (2, 1, 3, 0)
CHUNKS = 6
UNROLL = 3
F32, BF16 = jnp.float32, jnp.bfloat16
PLAIN = (((1,), (0,)), ((), ()))
TRANS_A = (((0,), (0,)), ((), ()))
TRANS_B = (((1,), (1,)), ((), ()))


def split(value):
    high = value.astype(BF16)
    return high, (value - high.astype(F32)).astype(BF16)


def dot(a, b, dims=PLAIN):
    return lax.dot_general(a, b, dims, preferred_element_type=F32)


def kernel(
    domain, ranks, slots_in, panels_in, transforms_in, trial_in, out,
    panels, transforms, trial,
    recv0, recv1, recv2, recv3, stage, slots_v, slots_s, dall, gram,
    kown, ksend, krecv, sig_f, sig_b, zrecv,
    in_sem, send_sem, recv_sem, slot_send, slot_recv, slot_local,
    ds_sem, dr_sem, rs_sem, rr_sem, ls_sem, lr_sem,
    ks_sem, kr_sem, zs_sem, zr_sem,
):
    pairs, piece, rank = out.shape[0], out.shape[2], out.shape[3]
    rows = panels.shape[1]
    lslot = domain.shape[0]
    width = transforms.shape[1]
    recvs = (recv0, recv1, recv2, recv3)
    pos = lax.axis_index("pairs")
    z = lax.axis_index("aux")
    x, y, c = pos // (2 * NY), (pos // 2) % NY, pos % 2

    loads = [
        pltpu.make_async_copy(src, dst, in_sem.at[n])
        for n, (src, dst) in enumerate(
            ((panels_in, panels), (transforms_in, transforms), (trial_in, trial))
        )
    ]
    for load in loads:
        load.start()

    def place(x2, y2, c2):
        return (x2 % NX) * (2 * NY) + (y2 % NY) * 2 + c2

    def same(m):
        return x + m * (1 - c), y + m * c, c

    def other(m):
        return x + m * c, y + m * (1 - c), 1 - c

    def other_source(m):
        return x + m * (1 - c), y + m * c, 1 - c

    def peer(r):
        return x + r * c, y + r * (1 - c), c

    def group_of(dest, r):
        x2, y2, c2 = dest
        return place(x2 + r * c2, y2 + r * (1 - c2), c2)

    barrier = pltpu.get_barrier_semaphore()
    greeted = 0
    for target in (
        [(place(*same(m)), z) for m in range(1, 4)]
        + [(place(*other(m)), z) for m in range(4)]
        + [(place(*other_source(m)), z) for m in range(1, 4)]
        + [(place(*peer(r)), z) for r in range(1, 4)]
        + [(pos, (z + k) % NZ) for k in (1, NZ - 1)]
    ):
        pl.semaphore_signal(barrier, inc=1, device_id=target, device_id_type=MESH)
        greeted += 1

    dests = [(same(m), 2 * m) for m in range(1, 4)] + [(other(m), 2 * m + 1) for m in range(4)]
    dests = [dests[k] for k in (1, 5, 0, 2, 4, 6, 3)]

    def fill(dest, r, k):
        group = group_of(dest, r)
        for s in range(lslot):
            stage[k, r, s] = panels[domain[s, group]]

    def panel_copy(dest, block, r, k):
        return pltpu.make_async_remote_copy(
            src_ref=stage.at[k, r],
            dst_ref=recvs[r].at[:, pl.ds(block * rows, rows), :],
            send_sem=send_sem.at[r, k],
            recv_sem=recv_sem.at[r, k],
            device_id=(place(*dest), z),
            device_id_type=MESH,
        )

    def slot_copy(r):
        return pltpu.make_async_remote_copy(
            src_ref=slots_in,
            dst_ref=slots_v.at[r],
            send_sem=slot_send.at[r],
            recv_sem=slot_recv.at[r],
            device_id=(place(*peer(NX - r)), z),
            device_id_type=MESH,
        )

    part = width // NZ

    def part_of(origin):
        return pl.ds(pl.multiple_of((origin % NZ) * part, part), part)

    def d_copy(r):
        return pltpu.make_async_remote_copy(
            src_ref=transforms.at[:, part_of(z), :],
            dst_ref=dall.at[r - 1, :, part_of(z), :],
            send_sem=ds_sem.at[r],
            recv_sem=dr_sem.at[r],
            device_id=(place(*peer(NX - r)), z),
            device_id_type=MESH,
        )

    half = pairs * ROOTS // 2

    def ring_copy(way, step, h):
        origin = part_of(z - way * step + NZ)
        chosen = slice(None)
        if step == NZ // 2 - 1:
            chosen = pl.ds(0, 2) if way == 1 else pl.ds(2, 1)
        send, recv = (rs_sem, rr_sem) if way == 1 else (ls_sem, lr_sem)
        ref = dall.at[chosen, pl.ds(h * half, half), origin, :]
        return pltpu.make_async_remote_copy(
            src_ref=ref,
            dst_ref=ref,
            send_sem=send.at[step, h],
            recv_sem=recv.at[step, h],
            device_id=(pos, (z + way + NZ) % NZ),
            device_id_type=MESH,
        )

    def ring(step, h):
        for way in (1, -1):
            if step:
                ring_copy(way, step - 1, h).wait_recv()
            if step < NZ // 2:
                ring_copy(way, step, h).start()

    work = [(r, k) for r in ORDER for k in range(len(dests))]
    loads[1].wait()
    pl.semaphore_wait(barrier, greeted)
    for r in (2, 1, 3):
        d_copy(r).start()
    for r in range(1, 4):
        slot_copy(r).start()
    loads[0].wait()
    for r, k in work:
        fill(dests[k][0], r, k)
    for r, k in work:
        if dests[k][1] % 2:
            panel_copy(*dests[k], r, k).start()
    for r in ORDER:
        group = group_of((x, y, c), r)
        for s in range(lslot):
            recvs[r][s, 0:rows, :] = panels[domain[s, group]]
    for r in range(1, 4):
        d_copy(r).wait_recv()
    ring(0, 0)
    ring(0, 1)
    for r, k in work:
        if dests[k][1] % 2 == 0:
            panel_copy(*dests[k], r, k).start()
    locals_ = [
        pltpu.make_async_copy(slots_v.at[r] if r else slots_in, slots_s.at[r], slot_local.at[r])
        for r in range(4)
    ]
    for r in range(4):
        if r:
            slot_copy(r).wait()
        locals_[r].start()
    for local in locals_:
        local.wait()
    loads[2].wait()

    def wait_panels(r):
        for k in range(len(dests)):
            panel_copy(*dests[k], r, k).wait_recv()

    def gram_of(r, p):
        left = recvs[r][slots_s[r, 0, p]]
        right = recvs[r][slots_s[r, 1, p]]
        gram[r, p] = dot(left, right, TRANS_A)

    def grams(r):
        def body(n, carry):
            for u in range(UNROLL):
                gram_of(r, n * UNROLL + u)
            return carry

        lax.fori_loop(0, pairs // UNROLL, body, 0)

    def k_of(r, p, d0, d1):
        g_high, g_low = split(gram[r, p])
        coeffs = jnp.concatenate([d0, d1], axis=1)
        t_high, t_low = split(dot(g_high, coeffs) + dot(g_low, coeffs))
        result = []
        for root, d in enumerate((d0, d1)):
            cols = slice(root * rank, (root + 1) * rank)
            both = jnp.concatenate([t_high[:, cols], t_low[:, cols]], axis=1)
            summed = dot(d, both, TRANS_A)
            result.append(summed[:, :rank] + summed[:, rank:])
        return result

    per = pairs // CHUNKS

    def k_copy(r, h):
        some = pl.ds(h * per, per)
        return pltpu.make_async_remote_copy(
            src_ref=ksend.at[r - 1, some],
            dst_ref=krecv.at[r - 1, some],
            send_sem=ks_sem.at[r - 1, h],
            recv_sem=kr_sem.at[r - 1, h],
            device_id=(place(*peer(r)), z),
            device_id_type=MESH,
        )

    def k_part(r, h):
        def body(chunk, carry):
            for n in range(per):
                p = chunk * per + n
                mats = k_of(r, p, dall[r - 1, ROOTS * p], dall[r - 1, ROOTS * p + 1])
                for root in range(ROOTS):
                    ksend[r - 1, p, root] = mats[root].astype(BF16)
            k_copy(r, chunk).start()
            return carry

        lax.fori_loop(h * CHUNKS // 2, (h + 1) * CHUNKS // 2, body, 0)

    ring(1, 0)
    ring(1, 1)
    wait_panels(2)
    ring(2, 0)
    grams(2)
    ring(2, 1)
    wait_panels(1)
    ring(3, 0)
    grams(1)
    ring(3, 1)
    ring(4, 0)
    k_part(2, 0)
    k_part(1, 0)
    wait_panels(3)
    grams(3)
    ring(4, 1)
    k_part(3, 0)
    k_part(2, 1)
    k_part(1, 1)
    k_part(3, 1)
    wait_panels(0)

    def z_copy(k, h):
        some = pl.ds(h * per, per)
        to = (z + k) % NZ
        return pltpu.make_async_remote_copy(
            src_ref=sig_b.at[some, :, pl.ds(pl.multiple_of(to * piece, piece), piece), :],
            dst_ref=zrecv.at[k, some],
            send_sem=zs_sem.at[k, h],
            recv_sem=zr_sem.at[k, h],
            device_id=(pos, to),
            device_id_type=MESH,
        )

    row_at = lax.broadcasted_iota(jnp.int32, (rank, rank), 0)
    col_at = lax.broadcasted_iota(jnp.int32, (rank, rank), 1)

    def sigma_chunk(h, carry):
        for n in range(per):
            gram_of(0, h * per + n)
        for n in range(per):
            p = h * per + n
            mats = k_of(0, p, transforms[ROOTS * p], transforms[ROOTS * p + 1])
            for root in range(ROOTS):
                kown[p, root] = mats[root]
        for r in range(1, 4):
            k_copy(r, h).wait_recv()
        for n in range(per):
            p = h * per + n
            for root in range(ROOTS):
                kmat = kown[p, root]
                for r in range(1, 4):
                    kmat = kmat + krecv[r - 1, p, root].astype(F32)
                keep = (row_at < ranks[root, p]) & (col_at < ranks[root, p])
                kmat = jnp.where(keep, kmat, 0.0)
                amp = jnp.where(keep, trial[p, root].astype(F32), 0.0).astype(BF16)
                both = jnp.concatenate(split(kmat), axis=1)
                sig = kmat + dot(both, jnp.concatenate([amp, amp], axis=0))
                sig = sig + dot(jnp.concatenate([amp, amp], axis=1), both, TRANS_B)
                sig_f[p, root] = sig
                sig_b[p, root] = sig.astype(BF16)
        for k in (4, 3, 5, 2, 6, 1, 7):
            z_copy(k, h).start()
        return carry

    lax.fori_loop(0, CHUNKS, sigma_chunk, 0)
    for r in ORDER:
        for k in range(len(dests)):
            panel_copy(*dests[k], r, k).wait_send()
    for r in range(1, 4):
        d_copy(r).wait_send()
        for h in range(CHUNKS):
            k_copy(r, h).wait_send()
    for step in range(NZ // 2):
        for way in (1, -1):
            for h in range(2):
                ring_copy(way, step, h).wait_send()

    def sum_chunk(h, carry):
        for k in range(1, NZ):
            z_copy(k, h).wait()
        for n in range(per):
            p = h * per + n
            for root in range(ROOTS):
                total = sig_f[p, root, pl.ds(pl.multiple_of(z * piece, piece), piece), :]
                for k in range(1, NZ):
                    total = total + zrecv[k, p, root].astype(F32)
                out[p, root] = total.astype(BF16)
        return carry

    lax.fori_loop(0, CHUNKS, sum_chunk, 0)


def per_device(panels, domain, pair_slots, ranks, transforms, trial):
    pairs, roots, width, rank = transforms.shape
    occ, rows, _ = panels.shape
    lslot = domain.shape[1]
    smem = pl.BlockSpec(memory_space=pltpu.SMEM)
    vmem = pl.BlockSpec(memory_space=pltpu.VMEM)
    far = pl.BlockSpec(memory_space=pl.ANY)
    dma = pltpu.SemaphoreType.DMA
    return pl.pallas_call(
        kernel,
        name="sigma",
        out_shape=jax.ShapeDtypeStruct((pairs, roots, rank // NZ, rank), BF16),
        in_specs=[smem, smem, vmem, far, far, far],
        out_specs=vmem,
        scratch_shapes=[
            pltpu.VMEM((occ, rows, width), BF16),
            pltpu.VMEM((pairs * roots, width, rank), BF16),
            pltpu.VMEM((pairs, roots, rank, rank), BF16),
        ]
        + [pltpu.VMEM((lslot, 8 * rows, width), BF16)] * 4
        + [
            pltpu.VMEM((7, 4, lslot, rows, width), BF16),
            pltpu.VMEM((4, 2, pairs), jnp.int32),
            pltpu.SMEM((4, 2, pairs), jnp.int32),
            pltpu.VMEM((3, pairs * roots, width, rank), BF16),
            pltpu.VMEM((4, pairs, width, width), F32),
            pltpu.VMEM((pairs, roots, rank, rank), F32),
            pltpu.VMEM((3, pairs, roots, rank, rank), BF16),
            pltpu.VMEM((3, pairs, roots, rank, rank), BF16),
            pltpu.VMEM((pairs, roots, rank, rank), F32),
            pltpu.VMEM((pairs, roots, rank, rank), BF16),
            pltpu.VMEM((NZ, pairs, roots, rank // NZ, rank), BF16),
            dma((3,)),
            dma((4, 7)),
            dma((4, 7)),
            dma((4,)),
            dma((4,)),
            dma((4,)),
            dma((4,)),
            dma((4,)),
            dma((4, 2)),
            dma((4, 2)),
            dma((4, 2)),
            dma((4, 2)),
            dma((3, CHUNKS)),
            dma((3, CHUNKS)),
            dma((NZ, CHUNKS)),
            dma((NZ, CHUNKS)),
        ],
        compiler_params=pltpu.CompilerParams(
            collective_id=0, has_side_effects=True, vmem_limit_bytes=67043328
        ),
    )(
        domain.T,
        ranks.T,
        pair_slots.T,
        panels,
        transforms.reshape(pairs * roots, width, rank),
        trial,
    )


def solution(mesh):
    return jax.shard_map(
        per_device,
        mesh=mesh,
        in_specs=(
            P(None, ("pairs", "aux"), None),
            P(),
            P("pairs", None),
            P("pairs", None),
            P("pairs", None, None, None),
            P("pairs", None, None, None),
        ),
        out_specs=P("pairs", None, "aux", None),
        check_vma=False,
    )
```

```python
import jax
import jax.numpy as jnp
from jax import lax
from jax.experimental import pallas as pl
from jax.experimental.pallas import tpu as pltpu
from jax.sharding import PartitionSpec as P

MESH = pl.DeviceIdType.MESH
NX, NY, NZ = 4, 4, 8
ROOTS = 2
ORDER = (2, 1, 3, 0)
CHUNKS = 6
QUARTERS = 4
EARLY = 2
F32, BF16 = jnp.float32, jnp.bfloat16
PLAIN = (((1,), (0,)), ((), ()))
TRANS_A = (((0,), (0,)), ((), ()))
TRANS_B = (((1,), (1,)), ((), ()))


def split(value):
    high = value.astype(BF16)
    return high, (value - high.astype(F32)).astype(BF16)


def dot(a, b, dims=PLAIN):
    return lax.dot_general(a, b, dims, preferred_element_type=F32)


def kernel(
    domain, ranks, slots_in, panels_in, transforms_in, trial_in, out,
    panels, transforms, trial,
    recv0, recv1, recv2, recv3, stage, slots_v, slots_s, dall, gram,
    kown, ksend, krecv, sig_f, sig_b, zrecv,
    out_v, in_sem, send_sem, recv_sem, slot_send, slot_recv, slot_local,
    ds_sem, dr_sem, ring_sem, rr_sem, lr_sem,
    ks_sem, kr_sem, zs_sem, zr_sem, out_sem,
):
    pairs, piece, rank = out.shape[0], out.shape[2], out.shape[3]
    rows = panels.shape[1]
    lslot = domain.shape[0]
    width = transforms.shape[1]
    recvs = (recv0, recv1, recv2, recv3)
    pos = lax.axis_index("pairs")
    z = lax.axis_index("aux")
    x, y, c = pos // (2 * NY), (pos // 2) % NY, pos % 2

    def arrived(ref, sem):
        pltpu.make_async_copy(ref, ref, sem).wait()

    loads = [
        pltpu.make_async_copy(src, dst, in_sem.at[n])
        for n, (src, dst) in enumerate(
            ((panels_in, panels), (transforms_in, transforms), (trial_in, trial))
        )
    ]
    for load in loads:
        load.start()

    def place(x2, y2, c2):
        return (x2 % NX) * (2 * NY) + (y2 % NY) * 2 + c2

    def same(m):
        return x + m * (1 - c), y + m * c, c

    def other(m):
        return x + m * c, y + m * (1 - c), 1 - c

    def other_source(m):
        return x + m * (1 - c), y + m * c, 1 - c

    def peer(r):
        return x + r * c, y + r * (1 - c), c

    def group_of(dest, r):
        x2, y2, c2 = dest
        return place(x2 + r * c2, y2 + r * (1 - c2), c2)

    barrier = pltpu.get_barrier_semaphore()
    greeted = 0
    for target in (
        [(place(*same(m)), z) for m in range(1, 4)]
        + [(place(*other(m)), z) for m in range(4)]
        + [(place(*other_source(m)), z) for m in range(1, 4)]
        + [(place(*peer(r)), z) for r in range(1, 4)]
        + [(pos, (z + k) % NZ) for k in (1, NZ - 1)]
    ):
        pl.semaphore_signal(barrier, inc=1, device_id=target, device_id_type=MESH)
        greeted += 1

    dests = [(same(m), 2 * m) for m in range(1, 4)] + [(other(m), 2 * m + 1) for m in range(4)]
    dests = [dests[k] for k in (1, 5, 0, 2, 4, 6, 3)]

    def fill(dest, r, k):
        group = group_of(dest, r)
        for s in range(lslot):
            stage[k, r, s] = panels[domain[s, group]]

    def panel_copy(dest, block, r, k):
        return pltpu.make_async_remote_copy(
            src_ref=stage.at[k, r],
            dst_ref=recvs[r].at[:, pl.ds(block * rows, rows), :],
            send_sem=send_sem,
            recv_sem=recv_sem.at[r],
            device_id=(place(*dest), z),
            device_id_type=MESH,
        )

    def slot_copy(r):
        return pltpu.make_async_remote_copy(
            src_ref=slots_in,
            dst_ref=slots_v.at[r],
            send_sem=slot_send.at[r],
            recv_sem=slot_recv.at[r],
            device_id=(place(*peer(NX - r)), z),
            device_id_type=MESH,
        )

    part = width // NZ

    def part_of(origin):
        return pl.ds(pl.multiple_of((origin % NZ) * part, part), part)

    def d_copy(r):
        return pltpu.make_async_remote_copy(
            src_ref=transforms.at[:, part_of(z), :],
            dst_ref=dall.at[r - 1, :, part_of(z), :],
            send_sem=ds_sem,
            recv_sem=dr_sem,
            device_id=(place(*peer(NX - r)), z),
            device_id_type=MESH,
        )

    quarter = pairs // QUARTERS

    def ring_copy(way, step, h):
        origin = part_of(z - way * step + NZ)
        chosen = slice(None)
        if step == NZ // 2 - 1:
            chosen = pl.ds(0, 2) if way == 1 else pl.ds(2, 1)
        recv = rr_sem if way == 1 else lr_sem
        ref = dall.at[chosen, pl.ds(h * quarter * ROOTS, quarter * ROOTS), origin, :]
        return pltpu.make_async_remote_copy(
            src_ref=ref,
            dst_ref=ref,
            send_sem=ring_sem,
            recv_sem=recv.at[step, h],
            device_id=(pos, (z + way + NZ) % NZ),
            device_id_type=MESH,
        )

    def ring(step, h):
        for way in (1, -1):
            if step:
                ring_copy(way, step - 1, h).wait_recv()
            if step < NZ // 2:
                ring_copy(way, step, h).start()

    work = [(r, k) for r in ORDER for k in range(len(dests))]
    loads[1].wait()
    pl.semaphore_wait(barrier, greeted)
    for r in (2, 1, 3):
        d_copy(r).start()
    for r in range(1, 4):
        slot_copy(r).start()
    loads[0].wait()
    for r, k in work:
        fill(dests[k][0], r, k)
    for r, k in work:
        if dests[k][1] % 2:
            panel_copy(*dests[k], r, k).start()
    for r in ORDER:
        group = group_of((x, y, c), r)
        for s in range(lslot):
            recvs[r][s, 0:rows, :] = panels[domain[s, group]]
    arrived(dall.at[:, :, part_of(z), :], dr_sem)
    ring(0, 0)
    ring(0, 1)
    for r, k in work:
        if dests[k][1] % 2 == 0:
            panel_copy(*dests[k], r, k).start()
    mine = pltpu.make_async_copy(slots_in, slots_s.at[0], slot_local.at[0])
    theirs = pltpu.make_async_copy(
        slots_v.at[pl.ds(1, 3)], slots_s.at[pl.ds(1, 3)], slot_local.at[1]
    )
    mine.start()
    for r in range(1, 4):
        slot_copy(r).wait()
    theirs.start()
    theirs.wait()
    mine.wait()
    loads[2].wait()

    def wait_panels(r):
        arrived(recvs[r].at[:, pl.ds(rows, 7 * rows), :], recv_sem.at[r])

    def gram_of(r, p):
        left = recvs[r][slots_s[r, 0, p]]
        right = recvs[r][slots_s[r, 1, p]]
        gram[r, p] = dot(left, right, TRANS_A)

    def grams(r):
        def body(n, carry):
            for u in range(quarter):
                gram_of(r, n * quarter + u)
            return carry

        lax.fori_loop(0, QUARTERS, body, 0)

    def k_of(r, p, d0, d1):
        g_high, g_low = split(gram[r, p])
        coeffs = jnp.concatenate([d0, d1], axis=1)
        t_high, t_low = split(dot(g_high, coeffs) + dot(g_low, coeffs))
        result = []
        for root, d in enumerate((d0, d1)):
            cols = slice(root * rank, (root + 1) * rank)
            both = jnp.concatenate([t_high[:, cols], t_low[:, cols]], axis=1)
            summed = dot(d, both, TRANS_A)
            result.append(summed[:, :rank] + summed[:, rank:])
        return result

    per = pairs // CHUNKS

    def k_copy(r, h):
        some = pl.ds(h * per, per)
        return pltpu.make_async_remote_copy(
            src_ref=ksend.at[r - 1, some],
            dst_ref=krecv.at[r - 1, some],
            send_sem=ks_sem,
            recv_sem=kr_sem.at[h],
            device_id=(place(*peer(r)), z),
            device_id_type=MESH,
        )

    def k_part(r, first, count=1):
        def body(q, carry):
            for n in range(quarter):
                p = q * quarter + n
                mats = k_of(r, p, dall[r - 1, ROOTS * p], dall[r - 1, ROOTS * p + 1])
                for root in range(ROOTS):
                    ksend[r - 1, p, root] = mats[root].astype(BF16)
            return carry

        lax.fori_loop(first, first + count, body, 0)

    def k_send(first, last):
        for h in range(first, last):
            for r in (2, 1, 3):
                k_copy(r, h).start()

    ring(1, 0)
    ring(1, 1)
    ring(2, 0)
    ring(2, 1)
    ring(3, 0)
    ring(0, 2)
    wait_panels(2)
    grams(2)
    ring(3, 1)
    ring(0, 3)
    ring(4, 0)
    k_part(2, 0)
    ring(1, 2)
    ring(4, 1)
    k_part(2, 1)
    ring(1, 3)
    wait_panels(1)
    ring(2, 2)
    grams(1)
    ring(2, 3)
    k_part(1, 0, 2)
    ring(3, 2)
    ring(3, 3)
    ring(4, 2)
    k_part(2, 2)
    wait_panels(3)
    grams(3)
    k_part(3, 0, 2)
    k_send(0, EARLY)
    k_part(1, 2)
    k_part(3, 2)
    ring(4, 3)
    k_part(2, 3)
    k_part(1, 3)
    k_part(3, 3)
    wait_panels(0)
    k_send(EARLY, CHUNKS)

    def z_copy(k, h):
        some = pl.ds(h * per, per)
        to = (z + k) % NZ
        return pltpu.make_async_remote_copy(
            src_ref=sig_b.at[some, :, pl.ds(pl.multiple_of(to * piece, piece), piece), :],
            dst_ref=zrecv.at[k, some],
            send_sem=zs_sem,
            recv_sem=zr_sem.at[h],
            device_id=(pos, to),
            device_id_type=MESH,
        )

    row_at = lax.broadcasted_iota(jnp.int32, (rank, rank), 0)
    col_at = lax.broadcasted_iota(jnp.int32, (rank, rank), 1)

    def sigma_chunk(h, carry):
        for n in range(per):
            gram_of(0, h * per + n)
        for n in range(per):
            p = h * per + n
            mats = k_of(0, p, transforms[ROOTS * p], transforms[ROOTS * p + 1])
            for root in range(ROOTS):
                kown[p, root] = mats[root]
        arrived(krecv.at[:, pl.ds(h * per, per)], kr_sem.at[h])
        for n in range(per):
            p = h * per + n
            for root in range(ROOTS):
                kmat = kown[p, root]
                for r in range(1, 4):
                    kmat = kmat + krecv[r - 1, p, root].astype(F32)
                keep = (row_at < ranks[root, p]) & (col_at < ranks[root, p])
                kmat = jnp.where(keep, kmat, 0.0)
                amp = jnp.where(keep, trial[p, root].astype(F32), 0.0).astype(BF16)
                both = jnp.concatenate(split(kmat), axis=1)
                sig = kmat + dot(both, jnp.concatenate([amp, amp], axis=0))
                sig = sig + dot(jnp.concatenate([amp, amp], axis=1), both, TRANS_B)
                sig_f[p, root] = sig
                sig_b[p, root] = sig.astype(BF16)
        for k in (4, 3, 5, 2, 6, 1, 7):
            z_copy(k, h).start()
        return carry

    lax.fori_loop(0, CHUNKS, sigma_chunk, 0)
    arrived(stage, send_sem)
    arrived(dall.at[:, :, part_of(z), :], ds_sem)
    arrived(dall.at[:, :, pl.ds(0, (NZ - 1) * part), :], ring_sem)
    arrived(ksend, ks_sem)

    def out_copy(some):
        return pltpu.make_async_copy(out_v.at[some], out.at[some], out_sem)

    def sum_chunk(h, carry):
        arrived(zrecv.at[pl.ds(1, NZ - 1), pl.ds(h * per, per)], zr_sem.at[h])
        for n in range(per):
            p = h * per + n
            for root in range(ROOTS):
                total = sig_f[p, root, pl.ds(pl.multiple_of(z * piece, piece), piece), :]
                for k in range(1, NZ):
                    total = total + zrecv[k, p, root].astype(F32)
                out_v[p, root] = total.astype(BF16)
        out_copy(pl.ds(h * per, per)).start()
        return carry

    lax.fori_loop(0, CHUNKS, sum_chunk, 0)
    arrived(zrecv.at[pl.ds(1, NZ - 1)], zs_sem)
    arrived(out_v, out_sem)


def per_device(panels, domain, pair_slots, ranks, transforms, trial):
    pairs, roots, width, rank = transforms.shape
    occ, rows, _ = panels.shape
    lslot = domain.shape[1]
    smem = pl.BlockSpec(memory_space=pltpu.SMEM)
    vmem = pl.BlockSpec(memory_space=pltpu.VMEM)
    far = pl.BlockSpec(memory_space=pl.ANY)
    dma = pltpu.SemaphoreType.DMA
    return pl.pallas_call(
        kernel,
        name="sigma",
        out_shape=jax.ShapeDtypeStruct((pairs, roots, rank // NZ, rank), BF16),
        in_specs=[smem, smem, vmem, far, far, far],
        out_specs=far,
        scratch_shapes=[
            pltpu.VMEM((occ, rows, width), BF16),
            pltpu.VMEM((pairs * roots, width, rank), BF16),
            pltpu.VMEM((pairs, roots, rank, rank), BF16),
        ]
        + [pltpu.VMEM((lslot, 8 * rows, width), BF16)] * 4
        + [
            pltpu.VMEM((7, 4, lslot, rows, width), BF16),
            pltpu.VMEM((4, 2, pairs), jnp.int32),
            pltpu.SMEM((4, 2, pairs), jnp.int32),
            pltpu.VMEM((3, pairs * roots, width, rank), BF16),
            pltpu.VMEM((4, pairs, width, width), F32),
            pltpu.VMEM((pairs, roots, rank, rank), F32),
            pltpu.VMEM((3, pairs, roots, rank, rank), BF16),
            pltpu.VMEM((3, pairs, roots, rank, rank), BF16),
            pltpu.VMEM((pairs, roots, rank, rank), F32),
            pltpu.VMEM((pairs, roots, rank, rank), BF16),
            pltpu.VMEM((NZ, pairs, roots, rank // NZ, rank), BF16),
            pltpu.VMEM((pairs, roots, rank // NZ, rank), BF16),
            dma((3,)),
            dma,
            dma((4,)),
            dma((4,)),
            dma((4,)),
            dma((2,)),
            dma,
            dma,
            dma,
            dma((NZ // 2, QUARTERS)),
            dma((NZ // 2, QUARTERS)),
            dma,
            dma((CHUNKS,)),
            dma,
            dma((CHUNKS,)),
            dma,
        ],
        compiler_params=pltpu.CompilerParams(
            collective_id=0, has_side_effects=True, vmem_limit_bytes=67043328
        ),
    )(
        domain.T,
        ranks.T,
        pair_slots.T,
        panels,
        transforms.reshape(pairs * roots, width, rank),
        trial,
    )


def solution(mesh):
    return jax.shard_map(
        per_device,
        mesh=mesh,
        in_specs=(
            P(None, ("pairs", "aux"), None),
            P(),
            P("pairs", None),
            P("pairs", None),
            P("pairs", None, None, None),
            P("pairs", None, None, None),
        ),
        out_specs=P("pairs", None, "aux", None),
        check_vma=False,
    )
```

```python
import jax
import jax.numpy as jnp
from jax import lax
from jax.experimental import pallas as pl
from jax.experimental.pallas import tpu as pltpu
from jax.sharding import PartitionSpec as P

MESH = pl.DeviceIdType.MESH
NX, NY, NZ = 4, 4, 8
ROOTS = 2
ORDER = (2, 1, 3, 0)
QUARTERS = 4
F32, BF16 = jnp.float32, jnp.bfloat16
PLAIN = (((1,), (0,)), ((), ()))
TRANS_A = (((0,), (0,)), ((), ()))
TRANS_B = (((1,), (1,)), ((), ()))


def split(value):
    high = value.astype(BF16)
    return high, (value - high.astype(F32)).astype(BF16)


def dot(a, b, dims=PLAIN):
    return lax.dot_general(a, b, dims, preferred_element_type=F32)


def kernel(
    domain_in, ranks_in, slots_in, panels_in, transforms_in, trial_in, out,
    domain, ranks, panels, transforms, trial,
    recv0, recv1, recv2, recv3, stage, slots_v, slots_s, dall, gram,
    keep_f, swap_out, swap_in, ysend, yrecv, sig_f, sig_b, zrecv,
    out_v, in_sem, send_sem, recv_sem, slot_send, slot_recv, slot_local,
    ds_sem, dr_sem, ring_sem, rr_sem, lr_sem,
    ws_sem, wr_sem, ys_sem, yr_sem, zs_sem, zr_sem, out_sem,
):
    pairs, piece, rank = out.shape[0], out.shape[2], out.shape[3]
    rows = panels.shape[1]
    lslot = domain.shape[0]
    width = transforms.shape[1]
    recvs = (recv0, recv1, recv2, recv3)
    pos = lax.axis_index("pairs")
    z = lax.axis_index("aux")
    x, y, c = pos // (2 * NY), (pos // 2) % NY, pos % 2

    def arrived(ref, sem):
        pltpu.make_async_copy(ref, ref, sem).wait()

    def place(x2, y2, c2):
        return (x2 % NX) * (2 * NY) + (y2 % NY) * 2 + c2

    def same(m):
        return x + m * (1 - c), y + m * c, c

    def other(m):
        return x + m * c, y + m * (1 - c), 1 - c

    def other_source(m):
        return x + m * (1 - c), y + m * c, 1 - c

    def peer(r):
        return x + r * c, y + r * (1 - c), c

    def group_of(dest, r):
        x2, y2, c2 = dest
        return place(x2 + r * c2, y2 + r * (1 - c2), c2)

    barrier = pltpu.get_barrier_semaphore()
    greeted = 0
    for target in (
        [(place(*same(m)), z) for m in range(1, 4)]
        + [(place(*other(m)), z) for m in range(4)]
        + [(place(*other_source(m)), z) for m in range(1, 4)]
        + [(place(*peer(r)), z) for r in range(1, 4)]
        + [(pos, (z + k) % NZ) for k in (1, NZ - 1)]
    ):
        pl.semaphore_signal(barrier, inc=1, device_id=target, device_id_type=MESH)
        greeted += 1

    def load(src, dst, n):
        copy = pltpu.make_async_copy(src, dst, in_sem.at[n])
        copy.start()
        return copy

    slot_load = load(slots_in, slots_v.at[0], 0)
    domain_load = load(domain_in, domain, 1)
    transforms_load = load(transforms_in, transforms, 2)
    panels_load = load(panels_in, panels, 3)
    late_loads = load(ranks_in, ranks, 4), load(trial_in, trial, 5)

    dests = [(same(m), 2 * m) for m in range(1, 4)] + [(other(m), 2 * m + 1) for m in range(4)]
    dests = [dests[k] for k in (1, 5, 0, 2, 4, 6, 3)]

    def fill(dest, r, k):
        group = group_of(dest, r)
        for s in range(lslot):
            stage[k, r, s] = panels[domain[s, group]]

    def panel_copy(dest, block, r, k):
        return pltpu.make_async_remote_copy(
            src_ref=stage.at[k, r],
            dst_ref=recvs[r].at[:, pl.ds(block * rows, rows), :],
            send_sem=send_sem,
            recv_sem=recv_sem.at[r],
            device_id=(place(*dest), z),
            device_id_type=MESH,
        )

    def slot_copy(r):
        return pltpu.make_async_remote_copy(
            src_ref=slots_v.at[0],
            dst_ref=slots_v.at[r],
            send_sem=slot_send.at[r],
            recv_sem=slot_recv.at[r],
            device_id=(place(*peer(NX - r)), z),
            device_id_type=MESH,
        )

    part = width // NZ

    def part_of(origin):
        return pl.ds(pl.multiple_of((origin % NZ) * part, part), part)

    def d_copy(r):
        return pltpu.make_async_remote_copy(
            src_ref=transforms.at[:, part_of(z), :],
            dst_ref=dall.at[r - 1, :, part_of(z), :],
            send_sem=ds_sem,
            recv_sem=dr_sem,
            device_id=(place(*peer(NX - r)), z),
            device_id_type=MESH,
        )

    quarter = pairs // QUARTERS

    def ring_copy(way, step, h):
        origin = part_of(z - way * step + NZ)
        chosen = slice(None)
        if step == NZ // 2 - 1:
            chosen = pl.ds(0, 2) if way == 1 else pl.ds(2, 1)
        recv = rr_sem if way == 1 else lr_sem
        ref = dall.at[chosen, pl.ds(h * quarter * ROOTS, quarter * ROOTS), origin, :]
        return pltpu.make_async_remote_copy(
            src_ref=ref,
            dst_ref=ref,
            send_sem=ring_sem,
            recv_sem=recv.at[step, h],
            device_id=(pos, (z + way + NZ) % NZ),
            device_id_type=MESH,
        )

    def ring(step, h):
        for way in (1, -1):
            if step:
                ring_copy(way, step - 1, h).wait_recv()
            if step < NZ // 2:
                ring_copy(way, step, h).start()

    work = [(r, k) for r in ORDER for k in range(len(dests))]
    slot_load.wait()
    transforms_load.wait()
    domain_load.wait()
    pl.semaphore_wait(barrier, greeted)
    for r in (2, 1, 3):
        d_copy(r).start()
    for r in range(1, 4):
        slot_copy(r).start()
    panels_load.wait()
    for r, k in work:
        fill(dests[k][0], r, k)
    for r, k in work:
        if dests[k][1] % 2:
            panel_copy(*dests[k], r, k).start()
    for r in ORDER:
        group = group_of((x, y, c), r)
        for s in range(lslot):
            recvs[r][s, 0:rows, :] = panels[domain[s, group]]
    arrived(dall.at[:, :, part_of(z), :], dr_sem)
    ring(0, 0)
    ring(0, 1)
    for r, k in work:
        if dests[k][1] % 2 == 0:
            panel_copy(*dests[k], r, k).start()
    for r in range(1, 4):
        slot_copy(r).wait()
    to_smem = pltpu.make_async_copy(slots_v, slots_s, slot_local)
    to_smem.start()
    to_smem.wait()
    for copy in late_loads:
        copy.wait()

    def wait_panels(r):
        arrived(recvs[r].at[:, pl.ds(rows, 7 * rows), :], recv_sem.at[r])

    def gram_of(r, p):
        left = recvs[r][slots_s[r, 0, p]]
        right = recvs[r][slots_s[r, 1, p]]
        gram[r, p] = dot(left, right, TRANS_A)

    def grams(r):
        def body(n, carry):
            for u in range(quarter):
                gram_of(r, n * quarter + u)
            return carry

        lax.fori_loop(0, QUARTERS, body, 0)

    def k_of(r, p, d0, d1):
        g_high, g_low = split(gram[r, p])
        coeffs = jnp.concatenate([d0, d1], axis=1)
        t_high, t_low = split(dot(g_high, coeffs) + dot(g_low, coeffs))
        result = []
        for root, d in enumerate((d0, d1)):
            cols = slice(root * rank, (root + 1) * rank)
            both = jnp.concatenate([t_high[:, cols], t_low[:, cols]], axis=1)
            summed = dot(d, both, TRANS_A)
            result.append(summed[:, :rank] + summed[:, rank:])
        return result

    side = (z + c) % 2
    partner = (z + 1 - 2 * side + NZ) % NZ

    def pair_at(chunk, mine, n):
        owner = side if mine else 1 - side
        return (2 * chunk + owner) * quarter + n

    def chunk_of(chunk):
        return pl.ds(chunk * quarter, quarter)

    def swap_copy(r, chunk):
        return pltpu.make_async_remote_copy(
            src_ref=swap_out.at[r, chunk_of(chunk)],
            dst_ref=swap_in.at[r, chunk_of(chunk)],
            send_sem=ws_sem,
            recv_sem=wr_sem.at[r, chunk],
            device_id=(pos, partner),
            device_id_type=MESH,
        )

    def y_copy(r, chunk):
        return pltpu.make_async_remote_copy(
            src_ref=ysend.at[r - 1, chunk_of(chunk)],
            dst_ref=yrecv.at[r - 1, chunk_of(chunk)],
            send_sem=ys_sem,
            recv_sem=yr_sem.at[chunk],
            device_id=(place(*peer(r)), z),
            device_id_type=MESH,
        )

    def k_quarter(r, chunk, mine):
        for n in range(quarter):
            p = pair_at(chunk, mine, n)
            source = dall.at[r - 1] if r else transforms
            mats = k_of(r, p, source[ROOTS * p], source[ROOTS * p + 1])
            for root in range(ROOTS):
                if mine:
                    keep_f[r, chunk * quarter + n, root] = mats[root]
                else:
                    swap_out[r, chunk * quarter + n, root] = mats[root].astype(BF16)

    def k_both(r, chunk):
        k_quarter(r, chunk, False)
        swap_copy(r, chunk).start()
        k_quarter(r, chunk, True)

    def own(chunk, mine):
        for n in range(quarter):
            gram_of(0, pair_at(chunk, mine, n))
        k_quarter(0, chunk, mine)
        if not mine:
            swap_copy(0, chunk).start()

    def merge(r, chunk):
        swap_copy(r, chunk).wait_recv()
        for n in range(quarter):
            at = chunk * quarter + n
            for root in range(ROOTS):
                summed = keep_f[r, at, root] + swap_in[r, at, root].astype(F32)
                ysend[r - 1, at, root] = summed.astype(BF16)
        y_copy(r, chunk).start()

    ring(1, 0)
    ring(1, 1)
    ring(2, 0)
    ring(2, 1)
    ring(3, 0)
    ring(0, 2)
    wait_panels(2)
    grams(2)
    ring(3, 1)
    ring(0, 3)
    ring(4, 0)
    ring(1, 2)
    ring(4, 1)
    ring(1, 3)
    k_both(2, 0)
    wait_panels(1)
    ring(2, 2)
    grams(1)
    ring(2, 3)
    k_both(1, 0)
    ring(3, 2)
    ring(3, 3)
    wait_panels(3)
    grams(3)
    ring(4, 2)
    k_both(3, 0)
    ring(4, 3)
    k_both(2, 1)
    k_both(1, 1)
    k_both(3, 1)
    merge(2, 0)
    merge(1, 0)
    merge(3, 0)
    wait_panels(0)
    own(0, False)
    own(1, False)
    merge(2, 1)
    merge(1, 1)
    merge(3, 1)
    own(0, True)

    def z_copy(k, chunk):
        to = (z + k) % NZ
        return pltpu.make_async_remote_copy(
            src_ref=sig_b.at[chunk_of(chunk), :, pl.ds(pl.multiple_of(to * piece, piece), piece), :],
            dst_ref=zrecv.at[k, chunk_of(chunk)],
            send_sem=zs_sem,
            recv_sem=zr_sem.at[chunk],
            device_id=(pos, to),
            device_id_type=MESH,
        )

    row_at = lax.broadcasted_iota(jnp.int32, (rank, rank), 0)
    col_at = lax.broadcasted_iota(jnp.int32, (rank, rank), 1)

    def sigmas(chunk):
        swap_copy(0, chunk).wait_recv()
        arrived(yrecv.at[:, chunk_of(chunk)], yr_sem.at[chunk])
        for n in range(quarter):
            at = chunk * quarter + n
            p = pair_at(chunk, True, n)
            for root in range(ROOTS):
                kmat = keep_f[0, at, root] + swap_in[0, at, root].astype(F32)
                for r in range(1, 4):
                    kmat = kmat + yrecv[r - 1, at, root].astype(F32)
                keep = (row_at < ranks[root, p]) & (col_at < ranks[root, p])
                kmat = jnp.where(keep, kmat, 0.0)
                amp = jnp.where(keep, trial[p, root].astype(F32), 0.0).astype(BF16)
                both = jnp.concatenate(split(kmat), axis=1)
                sig = kmat + dot(both, jnp.concatenate([amp, amp], axis=0))
                sig = sig + dot(jnp.concatenate([amp, amp], axis=1), both, TRANS_B)
                sig_f[at, root] = sig
                sig_b[at, root] = sig.astype(BF16)
        for k in (4, 3, 5, 2, 6, 1, 7):
            z_copy(k, chunk).start()

    sigmas(0)
    own(1, True)
    sigmas(1)
    arrived(stage, send_sem)
    arrived(dall.at[:, :, part_of(z), :], ds_sem)
    arrived(dall.at[:, :, pl.ds(0, (NZ - 1) * part), :], ring_sem)
    arrived(swap_out, ws_sem)
    arrived(ysend, ys_sem)

    def out_copy(chunk):
        some = pl.ds(chunk * 2 * quarter, 2 * quarter)
        return pltpu.make_async_copy(out_v.at[some], out.at[some], out_sem)

    for chunk in range(2):
        arrived(zrecv.at[pl.ds(1, NZ - 1), chunk_of(chunk)], zr_sem.at[chunk])
        for n in range(quarter):
            at = chunk * quarter + n
            for root in range(ROOTS):
                total = sig_f[at, root, pl.ds(pl.multiple_of(z * piece, piece), piece), :]
                for k in range(2, NZ, 2):
                    total = total + zrecv[k, at, root].astype(F32)
                out_v[pair_at(chunk, True, n), root] = total.astype(BF16)
                total = zrecv[1, at, root].astype(F32)
                for k in range(3, NZ, 2):
                    total = total + zrecv[k, at, root].astype(F32)
                out_v[pair_at(chunk, False, n), root] = total.astype(BF16)
        out_copy(chunk).start()
    arrived(zrecv.at[pl.ds(1, NZ - 1)], zs_sem)
    arrived(out_v, out_sem)


def per_device(panels, domain, pair_slots, ranks, transforms, trial):
    pairs, roots, width, rank = transforms.shape
    occ, rows, _ = panels.shape
    lslot = domain.shape[1]
    half = pairs // 2
    far = pl.BlockSpec(memory_space=pl.ANY)
    dma = pltpu.SemaphoreType.DMA
    return pl.pallas_call(
        kernel,
        name="sigma",
        out_shape=jax.ShapeDtypeStruct((pairs, roots, rank // NZ, rank), BF16),
        in_specs=[far] * 6,
        out_specs=far,
        scratch_shapes=[
            pltpu.SMEM(domain.shape[::-1], jnp.int32),
            pltpu.SMEM((roots, pairs), jnp.int32),
            pltpu.VMEM((occ, rows, width), BF16),
            pltpu.VMEM((pairs * roots, width, rank), BF16),
            pltpu.VMEM((pairs, roots, rank, rank), BF16),
        ]
        + [pltpu.VMEM((lslot, 8 * rows, width), BF16)] * 4
        + [
            pltpu.VMEM((7, 4, lslot, rows, width), BF16),
            pltpu.VMEM((4, 2, pairs), jnp.int32),
            pltpu.SMEM((4, 2, pairs), jnp.int32),
            pltpu.VMEM((3, pairs * roots, width, rank), BF16),
            pltpu.VMEM((4, pairs, width, width), F32),
            pltpu.VMEM((4, half, roots, rank, rank), F32),
            pltpu.VMEM((4, half, roots, rank, rank), BF16),
            pltpu.VMEM((4, half, roots, rank, rank), BF16),
            pltpu.VMEM((3, half, roots, rank, rank), BF16),
            pltpu.VMEM((3, half, roots, rank, rank), BF16),
            pltpu.VMEM((half, roots, rank, rank), F32),
            pltpu.VMEM((half, roots, rank, rank), BF16),
            pltpu.VMEM((NZ, half, roots, rank // NZ, rank), BF16),
            pltpu.VMEM((pairs, roots, rank // NZ, rank), BF16),
            dma((6,)),
            dma,
            dma((4,)),
            dma((4,)),
            dma((4,)),
            dma,
            dma,
            dma,
            dma,
            dma((NZ // 2, QUARTERS)),
            dma((NZ // 2, QUARTERS)),
            dma,
            dma((4, 2)),
            dma,
            dma((2,)),
            dma,
            dma((2,)),
            dma,
        ],
        compiler_params=pltpu.CompilerParams(
            collective_id=0, has_side_effects=True, vmem_limit_bytes=67043328
        ),
    )(
        domain.T,
        ranks.T,
        pair_slots.T,
        panels,
        transforms.reshape(pairs * roots, width, rank),
        trial,
    )


def solution(mesh):
    return jax.shard_map(
        per_device,
        mesh=mesh,
        in_specs=(
            P(None, ("pairs", "aux"), None),
            P(),
            P("pairs", None),
            P("pairs", None),
            P("pairs", None, None, None),
            P("pairs", None, None, None),
        ),
        out_specs=P("pairs", None, "aux", None),
        check_vma=False,
    )
```

```python
import jax
import jax.numpy as jnp
from jax import lax
from jax.experimental import pallas as pl
from jax.experimental.pallas import tpu as pltpu
from jax.sharding import PartitionSpec as P

MESH = pl.DeviceIdType.MESH
NX, NY, NZ = 4, 4, 8
ROOTS = 2
ORDER = (2, 1, 3, 0)
QUARTERS = 4
F32, BF16 = jnp.float32, jnp.bfloat16
PLAIN = (((1,), (0,)), ((), ()))
TRANS_A = (((0,), (0,)), ((), ()))
TRANS_B = (((1,), (1,)), ((), ()))


def split(value):
    high = value.astype(BF16)
    return high, (value - high.astype(F32)).astype(BF16)


def dot(a, b, dims=PLAIN):
    return lax.dot_general(a, b, dims, preferred_element_type=F32)


def kernel(
    domain_in, ranks_in, slots_in, panels_in, transforms_in, trial_in, out,
    domain, ranks, panels, transforms, trial,
    recv0, recv1, recv2, recv3, stage, slots_v, slots_s, dall, gram, half_t,
    keep_f, swap_out, swap_in, ysend, yrecv, sig_f, sig_b, zrecv,
    out_v, in_sem, send_sem, recv_sem, slot_send, slot_recv, slot_local,
    ds_sem, dr_sem, ring_sem, rr_sem, lr_sem,
    ws_sem, wr_sem, ys_sem, yr_sem, zs_sem, zr_sem, out_sem,
):
    pairs, piece, rank = out.shape[0], out.shape[2], out.shape[3]
    rows = panels.shape[1]
    lslot = domain.shape[0]
    width = transforms.shape[1]
    recvs = (recv0, recv1, recv2, recv3)
    pos = lax.axis_index("pairs")
    z = lax.axis_index("aux")
    x, y, c = pos // (2 * NY), (pos // 2) % NY, pos % 2

    def arrived(ref, sem):
        pltpu.make_async_copy(ref, ref, sem).wait()

    def place(x2, y2, c2):
        return (x2 % NX) * (2 * NY) + (y2 % NY) * 2 + c2

    def same(m):
        return x + m * (1 - c), y + m * c, c

    def other(m):
        return x + m * c, y + m * (1 - c), 1 - c

    def other_source(m):
        return x + m * (1 - c), y + m * c, 1 - c

    def peer(r):
        return x + r * c, y + r * (1 - c), c

    def group_of(dest, r):
        x2, y2, c2 = dest
        return place(x2 + r * c2, y2 + r * (1 - c2), c2)

    barrier = pltpu.get_barrier_semaphore()
    greeted = 0
    for target in (
        [(place(*same(m)), z) for m in range(1, 4)]
        + [(place(*other(m)), z) for m in range(4)]
        + [(place(*other_source(m)), z) for m in range(1, 4)]
        + [(place(*peer(r)), z) for r in range(1, 4)]
        + [(pos, (z + k) % NZ) for k in (1, NZ - 1)]
    ):
        pl.semaphore_signal(barrier, inc=1, device_id=target, device_id_type=MESH)
        greeted += 1

    def load(src, dst, n):
        copy = pltpu.make_async_copy(src, dst, in_sem.at[n])
        copy.start()
        return copy

    slot_load = load(slots_in, slots_v.at[0], 0)
    domain_load = load(domain_in, domain, 1)
    transforms_load = load(transforms_in, transforms, 2)
    panels_load = load(panels_in, panels, 3)
    late_loads = load(ranks_in, ranks, 4), load(trial_in, trial, 5)

    dests = [(same(m), 2 * m) for m in range(1, 4)] + [(other(m), 2 * m + 1) for m in range(4)]
    dests = [dests[k] for k in (1, 5, 0, 2, 4, 6, 3)]

    def fill(dest, r, k):
        group = group_of(dest, r)
        for s in range(lslot):
            stage[k, r, s] = panels[domain[s, group]]

    def panel_copy(dest, block, r, k):
        return pltpu.make_async_remote_copy(
            src_ref=stage.at[k, r],
            dst_ref=recvs[r].at[:, pl.ds(block * rows, rows), :],
            send_sem=send_sem,
            recv_sem=recv_sem.at[r],
            device_id=(place(*dest), z),
            device_id_type=MESH,
        )

    def slot_copy(r):
        return pltpu.make_async_remote_copy(
            src_ref=slots_v.at[0],
            dst_ref=slots_v.at[r],
            send_sem=slot_send.at[r],
            recv_sem=slot_recv.at[r],
            device_id=(place(*peer(NX - r)), z),
            device_id_type=MESH,
        )

    part = width // NZ

    def part_of(origin):
        return pl.ds(pl.multiple_of((origin % NZ) * part, part), part)

    def d_copy(r):
        return pltpu.make_async_remote_copy(
            src_ref=transforms.at[:, part_of(z), :],
            dst_ref=dall.at[r - 1, :, part_of(z), :],
            send_sem=ds_sem,
            recv_sem=dr_sem,
            device_id=(place(*peer(NX - r)), z),
            device_id_type=MESH,
        )

    quarter = pairs // QUARTERS

    def ring_copy(way, step, h):
        origin = part_of(z - way * step + NZ)
        chosen = slice(None)
        if step == NZ // 2 - 1:
            chosen = pl.ds(0, 2) if way == 1 else pl.ds(2, 1)
        recv = rr_sem if way == 1 else lr_sem
        ref = dall.at[chosen, pl.ds(h * quarter * ROOTS, quarter * ROOTS), origin, :]
        return pltpu.make_async_remote_copy(
            src_ref=ref,
            dst_ref=ref,
            send_sem=ring_sem,
            recv_sem=recv.at[step, h],
            device_id=(pos, (z + way + NZ) % NZ),
            device_id_type=MESH,
        )

    def ring(step, h):
        for way in (1, -1):
            if step:
                ring_copy(way, step - 1, h).wait_recv()
            if step < NZ // 2:
                ring_copy(way, step, h).start()

    work = [(r, k) for r in ORDER for k in range(len(dests))]
    slot_load.wait()
    transforms_load.wait()
    domain_load.wait()
    pl.semaphore_wait(barrier, greeted)
    for r in (2, 1, 3):
        d_copy(r).start()
    for r in range(1, 4):
        slot_copy(r).start()
    panels_load.wait()
    for r, k in work:
        fill(dests[k][0], r, k)
    for r, k in work:
        if dests[k][1] % 2:
            panel_copy(*dests[k], r, k).start()
    for r in ORDER:
        group = group_of((x, y, c), r)
        for s in range(lslot):
            recvs[r][s, 0:rows, :] = panels[domain[s, group]]
    arrived(dall.at[:, :, part_of(z), :], dr_sem)
    ring(0, 0)
    ring(0, 1)
    for r, k in work:
        if dests[k][1] % 2 == 0:
            panel_copy(*dests[k], r, k).start()
    for r in range(1, 4):
        slot_copy(r).wait()
    to_smem = pltpu.make_async_copy(slots_v, slots_s, slot_local)
    to_smem.start()
    to_smem.wait()
    for copy in late_loads:
        copy.wait()

    def wait_panels(r):
        arrived(recvs[r].at[:, pl.ds(rows, 7 * rows), :], recv_sem.at[r])

    def gram_of(r, p):
        left = recvs[r][slots_s[r, 0, p]]
        right = recvs[r][slots_s[r, 1, p]]
        gram[r, p] = dot(left, right, TRANS_A)

    def grams(r):
        def body(n, carry):
            for u in range(quarter):
                gram_of(r, n * quarter + u)
            return carry

        lax.fori_loop(0, QUARTERS, body, 0)

    side = (z + c) % 2
    partner = (z + 1 - 2 * side + NZ) % NZ

    def pair_at(chunk, mine, n):
        owner = side if mine else 1 - side
        return (2 * chunk + owner) * quarter + n

    def chunk_of(chunk):
        return pl.ds(chunk * quarter, quarter)

    def swap_copy(r, chunk):
        return pltpu.make_async_remote_copy(
            src_ref=swap_out.at[r, chunk_of(chunk)],
            dst_ref=swap_in.at[r, chunk_of(chunk)],
            send_sem=ws_sem,
            recv_sem=wr_sem.at[r, chunk],
            device_id=(pos, partner),
            device_id_type=MESH,
        )

    def y_copy(r, chunk):
        return pltpu.make_async_remote_copy(
            src_ref=ysend.at[r - 1, chunk_of(chunk)],
            dst_ref=yrecv.at[r - 1, chunk_of(chunk)],
            send_sem=ys_sem,
            recv_sem=yr_sem.at[chunk],
            device_id=(place(*peer(r)), z),
            device_id_type=MESH,
        )

    def k_quarters(r, quarters):
        source = dall.at[r - 1] if r else transforms
        todo = [(chunk, mine, n) for chunk, mine in quarters for n in range(quarter)]
        for slot, (chunk, mine, n) in enumerate(todo):
            p = pair_at(chunk, mine, n)
            coeffs = jnp.concatenate([source[ROOTS * p], source[ROOTS * p + 1]], axis=1)
            g_high, g_low = split(gram[r, p])
            t_high, t_low = split(dot(g_high, coeffs) + dot(g_low, coeffs))
            for root in range(ROOTS):
                cols = slice(root * rank, (root + 1) * rank)
                half_t[slot, root, :, 0:rank] = t_high[:, cols]
                half_t[slot, root, :, rank : 2 * rank] = t_low[:, cols]
        for slot, (chunk, mine, n) in enumerate(todo):
            p = pair_at(chunk, mine, n)
            for root in range(ROOTS):
                summed = dot(source[ROOTS * p + root], half_t[slot, root], TRANS_A)
                mat = summed[:, :rank] + summed[:, rank:]
                if mine:
                    keep_f[r, chunk * quarter + n, root] = mat
                else:
                    swap_out[r, chunk * quarter + n, root] = mat.astype(BF16)

    def k_both(r, chunk):
        k_quarters(r, [(chunk, False), (chunk, True)])
        swap_copy(r, chunk).start()

    def own(chunk, mine):
        for n in range(quarter):
            gram_of(0, pair_at(chunk, mine, n))
        k_quarters(0, [(chunk, mine)])
        if not mine:
            swap_copy(0, chunk).start()

    def merge(r, chunk):
        swap_copy(r, chunk).wait_recv()
        for n in range(quarter):
            at = chunk * quarter + n
            for root in range(ROOTS):
                summed = keep_f[r, at, root] + swap_in[r, at, root].astype(F32)
                ysend[r - 1, at, root] = summed.astype(BF16)
        y_copy(r, chunk).start()

    ring(1, 0)
    ring(1, 1)
    ring(2, 0)
    ring(2, 1)
    ring(3, 0)
    ring(0, 2)
    wait_panels(2)
    grams(2)
    ring(3, 1)
    ring(0, 3)
    ring(4, 0)
    ring(1, 2)
    ring(4, 1)
    ring(1, 3)
    k_both(2, 0)
    wait_panels(1)
    ring(2, 2)
    grams(1)
    ring(2, 3)
    k_both(1, 0)
    ring(3, 2)
    ring(3, 3)
    wait_panels(3)
    grams(3)
    ring(4, 2)
    k_both(3, 0)
    ring(4, 3)
    k_both(2, 1)
    k_both(1, 1)
    k_both(3, 1)
    wait_panels(0)
    merge(2, 0)
    merge(1, 0)
    merge(3, 0)
    own(0, False)
    own(1, False)
    merge(2, 1)
    merge(1, 1)
    merge(3, 1)
    own(0, True)
    own(1, True)

    def z_copy(k, chunk):
        to = (z + k) % NZ
        return pltpu.make_async_remote_copy(
            src_ref=sig_b.at[chunk_of(chunk), :, pl.ds(pl.multiple_of(to * piece, piece), piece), :],
            dst_ref=zrecv.at[k, chunk_of(chunk)],
            send_sem=zs_sem,
            recv_sem=zr_sem.at[chunk],
            device_id=(pos, to),
            device_id_type=MESH,
        )

    row_at = lax.broadcasted_iota(jnp.int32, (rank, rank), 0)
    col_at = lax.broadcasted_iota(jnp.int32, (rank, rank), 1)

    def sigmas(chunk):
        swap_copy(0, chunk).wait_recv()
        arrived(yrecv.at[:, chunk_of(chunk)], yr_sem.at[chunk])
        for n in range(quarter):
            at = chunk * quarter + n
            p = pair_at(chunk, True, n)
            for root in range(ROOTS):
                kmat = keep_f[0, at, root] + swap_in[0, at, root].astype(F32)
                for r in range(1, 4):
                    kmat = kmat + yrecv[r - 1, at, root].astype(F32)
                keep = (row_at < ranks[root, p]) & (col_at < ranks[root, p])
                kmat = jnp.where(keep, kmat, 0.0)
                amp = jnp.where(keep, trial[p, root].astype(F32), 0.0).astype(BF16)
                both = jnp.concatenate(split(kmat), axis=1)
                sig = kmat + dot(both, jnp.concatenate([amp, amp], axis=0))
                sig = sig + dot(jnp.concatenate([amp, amp], axis=1), both, TRANS_B)
                sig_f[at, root] = sig
                sig_b[at, root] = sig.astype(BF16)
        for k in (4, 3, 5, 2, 6, 1, 7):
            z_copy(k, chunk).start()

    sigmas(0)
    sigmas(1)
    arrived(stage, send_sem)
    arrived(dall.at[:, :, part_of(z), :], ds_sem)
    arrived(dall.at[:, :, pl.ds(0, (NZ - 1) * part), :], ring_sem)
    arrived(swap_out, ws_sem)
    arrived(ysend, ys_sem)

    def out_copy(chunk):
        some = pl.ds(chunk * 2 * quarter, 2 * quarter)
        return pltpu.make_async_copy(out_v.at[some], out.at[some], out_sem)

    for chunk in range(2):
        arrived(zrecv.at[pl.ds(1, NZ - 1), chunk_of(chunk)], zr_sem.at[chunk])
        for n in range(quarter):
            at = chunk * quarter + n
            for root in range(ROOTS):
                total = sig_f[at, root, pl.ds(pl.multiple_of(z * piece, piece), piece), :]
                for k in range(2, NZ, 2):
                    total = total + zrecv[k, at, root].astype(F32)
                out_v[pair_at(chunk, True, n), root] = total
                total = zrecv[1, at, root].astype(F32)
                for k in range(3, NZ, 2):
                    total = total + zrecv[k, at, root].astype(F32)
                out_v[pair_at(chunk, False, n), root] = total
        out_copy(chunk).start()
    arrived(zrecv.at[pl.ds(1, NZ - 1)], zs_sem)
    arrived(out_v, out_sem)


def per_device(panels, domain, pair_slots, ranks, transforms, trial):
    pairs, roots, width, rank = transforms.shape
    occ, rows, _ = panels.shape
    lslot = domain.shape[1]
    half = pairs // 2
    far = pl.BlockSpec(memory_space=pl.ANY)
    dma = pltpu.SemaphoreType.DMA
    return pl.pallas_call(
        kernel,
        name="sigma",
        out_shape=jax.ShapeDtypeStruct((pairs, roots, rank // NZ, rank), F32),
        in_specs=[far] * 6,
        out_specs=far,
        scratch_shapes=[
            pltpu.SMEM(domain.shape[::-1], jnp.int32),
            pltpu.SMEM((roots, pairs), jnp.int32),
            pltpu.VMEM((occ, rows, width), BF16),
            pltpu.VMEM((pairs * roots, width, rank), BF16),
            pltpu.VMEM((pairs, roots, rank, rank), BF16),
        ]
        + [pltpu.VMEM((lslot, 8 * rows, width), BF16)] * 4
        + [
            pltpu.VMEM((7, 4, lslot, rows, width), BF16),
            pltpu.VMEM((4, 2, pairs), jnp.int32),
            pltpu.SMEM((4, 2, pairs), jnp.int32),
            pltpu.VMEM((3, pairs * roots, width, rank), BF16),
            pltpu.VMEM((4, pairs, width, width), F32),
            pltpu.VMEM((half, roots, width, 2 * rank), BF16),
            pltpu.VMEM((4, half, roots, rank, rank), F32),
            pltpu.VMEM((4, half, roots, rank, rank), BF16),
            pltpu.VMEM((4, half, roots, rank, rank), BF16),
            pltpu.VMEM((3, half, roots, rank, rank), BF16),
            pltpu.VMEM((3, half, roots, rank, rank), BF16),
            pltpu.VMEM((half, roots, rank, rank), F32),
            pltpu.VMEM((half, roots, rank, rank), BF16),
            pltpu.VMEM((NZ, half, roots, rank // NZ, rank), BF16),
            pltpu.VMEM((pairs, roots, rank // NZ, rank), F32),
            dma((6,)),
            dma,
            dma((4,)),
            dma((4,)),
            dma((4,)),
            dma,
            dma,
            dma,
            dma,
            dma((NZ // 2, QUARTERS)),
            dma((NZ // 2, QUARTERS)),
            dma,
            dma((4, 2)),
            dma,
            dma((2,)),
            dma,
            dma((2,)),
            dma,
        ],
        compiler_params=pltpu.CompilerParams(
            collective_id=0, has_side_effects=True, vmem_limit_bytes=67043328
        ),
    )(
        domain.T,
        ranks.T,
        pair_slots.T,
        panels,
        transforms.reshape(pairs * roots, width, rank),
        trial,
    ).astype(BF16)


def solution(mesh):
    return jax.shard_map(
        per_device,
        mesh=mesh,
        in_specs=(
            P(None, ("pairs", "aux"), None),
            P(),
            P("pairs", None),
            P("pairs", None),
            P("pairs", None, None, None),
            P("pairs", None, None, None),
        ),
        out_specs=P("pairs", None, "aux", None),
        check_vma=False,
    )
```
